32 devices in a mesh: root: 4 (over x, core), virt: 8 (over z, y).
Axes of the slice: x: 2, y: 2, z: 4, core: 2. Of those that a mesh axis runs over, the one named last changes fastest.
Arguments:
- r2: bfloat16 [512, 16384], P('virt', 'root'), parts along dimension 1, may hold values from -6 to 6
- tau: bfloat16 [512, 512, 3072], P('virt', None, 'root'), parts along dimension 2, may hold values from -6 to 6
- w_vvv: bfloat16 [512, 512, 512], P('virt'), may hold values from -0.01171875 to 0.01171875
- w_oooo: bfloat16 [768, 4096], P('virt'), may hold values from -0.09375 to 0.09375
- w_ovoo: bfloat16 [64, 768, 512], P(None, 'virt'), may hold values from -0.75 to 0.75
- fock_oo: bfloat16 [64, 64], replicated, may hold values from -0.75 to 0.75
- fock_vv: bfloat16 [512, 512], replicated, may hold values from -0.25 to 0.25
- r1: bfloat16 [256], P('root'), parts along dimension 0, may hold values from -6 to 6
Outputs:
- sigma: float32 [3072, 512], P(('root', 'virt')), parts along dimension 0
The draws below stay inside these ranges and needn't reach their ends.
There are 4 independent parts, one for each index of `root`. The reference program is written for one: setup_inputs(seed, part) draws one part's arguments, and reference() takes and returns one part's arrays. A program takes and returns all parts, laid end to end along the dimension named above; an argument that names none is the same for every part. Nothing has to cross between parts.
All inputs are finite; a program needn't handle non-finite values.
Results may differ from the reference program's by a relative error of at most 0.0003.
Values may be sent and summed in bfloat16 or wider, within the bound.
No kernel may reach another device: no remote copies, remote signals or barrier semaphores. Data moves between devices by JAX's collectives and lax.ppermute only.
A program may use at most 256 MiB of HBM per device.

```python
import jax
import jax.numpy as jnp
from jax import lax

O = 64
V = 512
OI = 12
PAIRS = 768


def spiked(values, stream_key, source, target, blocks, factor):
    owner, partner = [(jnp.arange(values.shape[dim]) // (values.shape[dim] // blocks)).reshape([-1 if axis == dim else 1 for axis in range(values.ndim)]) for dim in (source, target)]
    chosen = jax.random.permutation(stream_key, blocks)[partner]
    strong = (owner == chosen) | (owner == (partner + blocks // 2) % blocks)
    return jnp.where(strong, factor * values, values)


def block_scale(key, extent, split, smallest, high):
    factor_of = 1.0
    for axis_at, blocks in split:
        heights = jax.random.uniform(jax.random.fold_in(jax.random.fold_in(key, 6), axis_at), (blocks,), jnp.float32, smallest / len(split), high / len(split))
        factor_of = factor_of * jnp.repeat(jnp.exp(heights), extent[axis_at] // blocks).reshape((-1,) + (1,) * (len(extent) - 1 - axis_at))
    return factor_of


def noise(own_key, shape, width, bound, cuts=(), kind=jnp.bfloat16):
    entries = jax.random.normal(own_key, shape, jnp.float32) * width
    if len(cuts) > 0:
        entries = block_scale(own_key, shape, cuts, -0.22, 0.18) * entries
    return jnp.clip(entries, min=-bound, max=bound).astype(kind)


def noise_with(key, extent, scale, limit, shards, heavy, dtype=jnp.bfloat16):
    result = scale * jax.random.normal(key, extent, jnp.float32)
    if shards:
        result = result * block_scale(key, extent, shards, -0.22, 0.18)
    return jnp.clip(spiked(result, jax.random.fold_in(key, 3), *heavy), -limit, limit).astype(dtype)


def setup_inputs(seed: int = 0, part: int = 0) -> dict:
    key_of = jax.random.split(jax.random.key(seed), 9)
    part_splits = jax.random.split(jax.random.fold_in(key_of[8], part), 9)
    r2 = noise(part_splits[0], (V, O * O), 1.0, 6.0, ((0, 8),))
    tau = noise_with(part_splits[1], (V, V, PAIRS), 1.0, 6.0, ((0, 8),), (0, 2, 8, 2.0))
    w_vvv = noise(key_of[2], (V, V, V), (V * V) ** -0.5, 0.01171875, ((0, 8),))
    w_oooo = noise(key_of[3], (PAIRS, O * O), (O * O) ** -0.5, 0.09375, ((0, 8),))
    w_ovoo = noise(key_of[4], (O, PAIRS, V), O ** -0.5, 0.75, ((1, 8),))
    fock_oo = noise(key_of[5], (O, O), O ** -0.5, 0.75)
    fock_vv = noise(key_of[6], (V, V), V ** -0.5, 0.25)
    r1 = noise(part_splits[7], (O,), 1.0, 6.0)
    return dict(r2=r2, tau=tau, w_vvv=w_vvv, w_oooo=w_oooo, w_ovoo=w_ovoo, fock_oo=fock_oo, fock_vv=fock_vv, r1=r1)


def reference(r2, tau, w_vvv, w_oooo, w_ovoo, fock_oo, fock_vv, r1):
    pair_count = OI * O
    tau_flat = tau.reshape(V * V, pair_count)
    weight_flat = jnp.transpose(w_vvv, (1, 0, 2)).reshape(V * V, V)
    three_virtual = jnp.dot(tau_flat.T, weight_flat, preferred_element_type=jnp.float32)
    window = r2[:, :pair_count]
    vv_term = jnp.dot(window.T, fock_vv.T, preferred_element_type=jnp.float32)
    oooo_term = jnp.dot(w_oooo, r2.T, preferred_element_type=jnp.float32)
    cubic_view = r2.astype(jnp.float32).reshape(V, O, O)
    fock_wide = fock_oo.astype(jnp.float32)
    first_term = jnp.einsum("mi,amj->aij", fock_wide, cubic_view, precision=lax.Precision.HIGHEST)
    second_term = jnp.einsum("mj,aim->aij", fock_wide, cubic_view, precision=lax.Precision.HIGHEST)
    occ_term = (first_term + second_term).reshape(V, O * O)[:, :pair_count].T
    singles_term = jnp.dot(r1[None, :], w_ovoo.reshape(O, pair_count * V), preferred_element_type=jnp.float32).reshape(pair_count, V)
    return three_virtual + vv_term + oooo_term - occ_term - singles_term
```

```python
import functools

import jax
import jax.numpy as jnp
import numpy as np
from jax import lax
from jax.experimental import pallas as pl
from jax.experimental.pallas import tpu as pltpu
from jax.sharding import PartitionSpec as P


PHASES = (((0, 6), (0, 4, 8, 12, 16)), ((6, 8), (0, 8, 12, 16)))


def chunks_of(columns, rows):
    found = []
    for (a0, a1), cuts in PHASES:
        cuts = sorted({c * rows // 16 for c in cuts})
        for f0, f1 in zip(cuts, cuts[1:]):
            found.append((a0 * columns // 8, a1 * columns // 8, f0, f1))
    return found


def swap(value, axis, size, bit):
    return lax.ppermute(value, axis, [(k, k ^ bit) for k in range(size)])


def spread(piece, size):
    held = {0: piece}
    bit = size // 2
    while bit:
        for key, part in list(held.items()):
            held[key ^ bit] = swap(part, "root", size, bit)
        bit //= 2
    return held


def scatter_sum(partial, size):
    place = lax.axis_index("virt")
    bit = 1
    while bit < size:
        parts = partial.reshape(partial.shape[0] // 2, 2, *partial.shape[1:])
        mine = (place // bit) % 2
        keep = lax.dynamic_index_in_dim(parts, mine, 1, keepdims=False)
        give = lax.dynamic_index_in_dim(parts, 1 - mine, 1, keepdims=False)
        partial = keep + swap(give, "virt", size, bit)
        bit *= 2
    return partial[0]


def pack_body(place_ref, select_ref, slab_ref, *out_refs, chunks):
    rows, span, columns = slab_ref.shape
    group = select_ref.shape[0] // span
    for g in range(0, rows, group):
        part = slab_ref[g : g + group].reshape(group * span, columns)
        moved = jnp.dot(select_ref[...], part, preferred_element_type=jnp.float32)
        moved = moved.astype(jnp.bfloat16).reshape(span, group, columns)
        for (a0, a1, f0, f1), out_ref in zip(chunks, out_refs):
            out_ref[0, :, g : g + group, :] = moved[f0:f1, :, a0:a1]


def pack(w_vvv, virts, roots, root, chunks):
    rows, total, columns = w_vvv.shape
    span = total // (virts * roots)
    group = 16
    if span % 16 or rows % group or any((a1 - a0) % 128 for a0, a1, _, _ in chunks):
        slab = w_vvv.reshape(rows, virts, roots, span, columns)
        slab = lax.dynamic_index_in_dim(slab, root, 2, keepdims=False).transpose(1, 2, 0, 3)
        return [slab[:, f0:f1, :, a0:a1] for a0, a1, f0, f1 in chunks]
    to = np.arange(span * group)[:, None]
    select = np.arange(span * group)[None] == to % group * span + to // group
    shapes = [(virts, f1 - f0, rows, a1 - a0) for a0, a1, f0, f1 in chunks]
    return pl.pallas_call(
        functools.partial(pack_body, chunks=chunks),
        grid_spec=pltpu.PrefetchScalarGridSpec(
            num_scalar_prefetch=1,
            grid=(virts,),
            in_specs=[
                pl.BlockSpec(select.shape, lambda i, q: (0, 0)),
                pl.BlockSpec((rows, span, columns), lambda i, q: (0, i * roots + q[0], 0)),
            ],
            out_specs=[pl.BlockSpec((1, *shape[1:]), lambda i, q: (i, 0, 0, 0)) for shape in shapes],
        ),
        out_shape=[jax.ShapeDtypeStruct(shape, w_vvv.dtype) for shape in shapes],
        cost_estimate=pl.CostEstimate(
            flops=2 * virts * span * rows * columns * span * group,
            bytes_accessed=4 * virts * rows * span * columns,
            transcendentals=0,
        ),
    )(root[None].astype(jnp.int32), jnp.asarray(select, w_vvv.dtype), w_vvv)


def ladder_body(place_ref, tau_ref, *refs, steps, count):
    pieces, out_ref = refs[:count], refs[-1]
    at = pl.program_id(0)

    @pl.when(at == 0)
    def _():
        out_ref[...] = refs[count][...] if len(refs) > count + 1 else jnp.zeros_like(out_ref)

    for k, piece_ref in enumerate(pieces):

        @pl.when(at // steps == k)
        def _(piece_ref=piece_ref):
            sources, taken, rows, columns = piece_ref.shape
            left = [piece_ref[:, f].reshape(sources * rows, columns) for f in range(taken)]
            left = jnp.concatenate(left, 0)
            right = tau_ref[...].reshape(left.shape[0], tau_ref.shape[-1])
            out_ref[...] += lax.dot_general(
                left, right, (((0,), (0,)), ((), ())), preferred_element_type=jnp.float32
            )


def ladder(tau, pieces, running, places, first, roots):
    sources, taken, rows, columns = pieces[0].shape
    total, pairs = tau.shape[1:]
    span = tau.shape[0] // roots
    count = len(pieces)
    step = 4
    while taken % step or first % step or span % step:
        step //= 2
    steps = taken // step
    whole = pl.BlockSpec((columns, pairs), lambda i, q: (0, 0))
    given = () if running is None else (running,)

    def piece_spec(k):
        return pl.BlockSpec(
            (sources, step, rows, columns),
            lambda i, q: (0, jnp.clip(i - k * steps, 0, steps - 1), 0, 0),
        )

    return pl.pallas_call(
        functools.partial(ladder_body, steps=steps, count=count),
        grid_spec=pltpu.PrefetchScalarGridSpec(
            num_scalar_prefetch=1,
            grid=(count * steps,),
            in_specs=[
                pl.BlockSpec(
                    (step, total, pairs),
                    lambda i, q: ((q[i // steps] * span + first) // step + i % steps, 0, 0),
                ),
                *[piece_spec(k) for k in range(count)],
                *[whole for _ in given],
            ],
            out_specs=whole,
        ),
        out_shape=jax.ShapeDtypeStruct((columns, pairs), jnp.float32),
        input_output_aliases={2 + count: 0} if given else {},
        cost_estimate=pl.CostEstimate(
            flops=2 * count * sources * taken * rows * columns * pairs,
            bytes_accessed=2 * count * sources * taken * rows * (columns + pairs),
            transcendentals=0,
        ),
    )(jnp.stack(places).astype(jnp.int32), tau, *pieces, *given)


def on_device(sizes, r2, tau, w_vvv, w_oooo, w_ovoo, fock_oo, fock_vv, r1):
    roots, virts = sizes["root"], sizes["virt"]
    root, virt = lax.axis_index("root"), lax.axis_index("virt")
    f32 = jnp.float32
    block, _, columns = w_vvv.shape
    fblock, _, pairs = tau.shape
    occupied = fock_oo.shape[0]
    pair_rows = w_oooo.shape[0]
    rq = pair_rows // roots

    chunks = chunks_of(columns, fblock // roots)
    sends = pack(w_vvv, virts, roots, root, chunks)
    arrived = []
    for send in sends:
        arrived.append(lax.all_to_all(send, "virt", 0, 0, tiled=True))

    own_rows = lax.dynamic_slice_in_dim(w_oooo, root * rq, rq, 0)
    small = jnp.concatenate([r2, own_rows], 0)
    inner = small.shape[1] // virts
    small = small.reshape(block + rq, virts, inner).transpose(1, 0, 2)
    r2_part = jnp.zeros((virts, block, inner), r2.dtype)
    rows_part = jnp.zeros((virts, rq, inner), r2.dtype)
    for key in range(virts):
        piece = lax.dynamic_index_in_dim(small, virt ^ key, 0)
        if key:
            piece = lax.ppermute(piece, "virt", [(k, k ^ key) for k in range(virts)])
        r2_part = lax.dynamic_update_slice(r2_part, piece[:, :block], (virt ^ key, 0, 0))
        rows_part = lax.dynamic_update_slice(rows_part, piece[:, block:], (virt ^ key, 0, 0))
    r2_part = r2_part.reshape(columns, inner)
    rows_of = spread(rows_part, roots)
    oooo_part = jnp.zeros((virts, roots, rq, inner), r2.dtype)
    for key, part in rows_of.items():
        oooo_part = lax.dynamic_update_slice(oooo_part, part[:, None], (0, root ^ key, 0, 0))
    oooo_part = oooo_part.reshape(pairs, inner)

    window = r2[:, :pairs]
    fock_cols = lax.dynamic_slice_in_dim(fock_vv, virt * block, block, 1)
    extra = jnp.einsum("ep,ae->pa", window, fock_cols, preferred_element_type=f32)
    outer = pairs // occupied
    cube = r2.reshape(block, occupied, occupied)
    first = jnp.einsum("mi,amj->aij", fock_oo[:, :outer], cube, preferred_element_type=f32)
    second = jnp.einsum("mj,aim->aij", fock_oo, cube[:, :outer], preferred_element_type=f32)
    occ = (first + second).reshape(block, pairs).T
    placed = lax.dynamic_update_slice(jnp.zeros((pairs, columns), f32), occ, (0, virt * block))
    extra = extra - placed
    extra = extra + jnp.einsum("pk,ak->pa", oooo_part, r2_part, preferred_element_type=f32)

    singles = jnp.dot(
        r1[None, :], w_ovoo.reshape(w_ovoo.shape[0], -1), preferred_element_type=f32
    ).reshape(pair_rows, -1)

    running = {}
    results = {}
    for index, (a0, a1, f0, f1) in enumerate(chunks):
        held = spread(arrived[index], roots)
        for keys in groups_of(index, len(chunks), roots):
            running[a0] = ladder(
                tau, [held[k] for k in keys], running.get(a0), [root ^ k for k in keys], f0, roots
            )
        if f1 == fblock // roots:
            partial = running[a0].T + extra[:, a0:a1]
            summed = scatter_sum(partial.reshape(virts, pair_rows, a1 - a0), virts)
            results[a0] = summed - singles[:, a0:a1]
    return jnp.concatenate([results[a0] for a0 in sorted(results)], 1)


def groups_of(index, count, roots):
    keys = list(range(roots))
    if index + 4 < count:
        return [keys]
    return [keys[: roots // 2], keys[roots // 2 :]]


def solution(mesh):
    sizes = dict(mesh.shape)
    in_specs = (
        P("virt", "root"),
        P("virt", None, "root"),
        P("virt", None, None),
        P("virt", None),
        P(None, "virt", None),
        P(),
        P(),
        P("root"),
    )
    out_specs = P(("root", "virt"), None)

    def body(*args):
        return on_device(sizes, *args)

    return jax.shard_map(
        body, mesh=mesh, in_specs=in_specs, out_specs=out_specs, check_vma=False
    )
```

```python
import functools

import jax
import jax.numpy as jnp
import numpy as np
from jax import lax
from jax.experimental import pallas as pl
from jax.experimental.pallas import tpu as pltpu
from jax.sharding import PartitionSpec as P


MAIN = ((0, 6, 0, 4), (0, 6, 4, 8), (0, 6, 8, 12), (0, 6, 12, 16), (6, 8, 12, 16))
SHADOW = ((6, 8, 0, 4), (6, 8, 4, 8), (6, 8, 8, 12), None, None)
SPLIT = 2


def chunks_of(columns, rows):
    found = {}
    for n, pair in enumerate(zip(MAIN, SHADOW)):
        for name, cut in zip((f"m{n}", f"q{n}"), pair):
            if cut is not None:
                a0, a1, f0, f1 = cut
                found[name] = (a0 * columns // 8, a1 * columns // 8, f0 * rows // 16, f1 * rows // 16)
    return {name: cut for name, cut in found.items() if cut[3] > cut[2]}


def swap(value, axis, size, bit):
    return lax.ppermute(value, axis, [(k, k ^ bit) for k in range(size)])


def spread(piece, size):
    held = {0: piece}
    bit = size // 2
    while bit:
        for key, part in list(held.items()):
            held[key ^ bit] = swap(part, "root", size, bit)
        bit //= 2
    return held


def scatter_sum(partial, size):
    place = lax.axis_index("virt")
    bit = 1
    while bit < size:
        parts = partial.reshape(partial.shape[0] // 2, 2, *partial.shape[1:])
        mine = (place // bit) % 2
        keep = lax.dynamic_index_in_dim(parts, mine, 1, keepdims=False)
        give = lax.dynamic_index_in_dim(parts, 1 - mine, 1, keepdims=False)
        partial = keep + swap(give, "virt", size, bit)
        bit *= 2
    return partial[0]


def assemble_body(place_ref, *refs):
    for k, ref in enumerate(refs[:-1]):

        @pl.when(pl.program_id(0) == k)
        def _(ref=ref):
            refs[-1][...] = ref[...]


def assemble(parts, place):
    shape = parts[0].shape
    rest = (0,) * (len(shape) - 1)
    return pl.pallas_call(
        assemble_body,
        grid_spec=pltpu.PrefetchScalarGridSpec(
            num_scalar_prefetch=1,
            grid=(len(parts),),
            in_specs=[pl.BlockSpec(shape, lambda i, q: (0, *rest)) for _ in parts],
            out_specs=pl.BlockSpec(shape, lambda i, q: (q[0] ^ i, *rest)),
        ),
        out_shape=jax.ShapeDtypeStruct((len(parts), *shape[1:]), parts[0].dtype),
    )(place[None].astype(jnp.int32), *parts)


def pack_body(place_ref, select_ref, slab_ref, *out_refs, chunks):
    rows, span, columns = slab_ref.shape
    group = select_ref.shape[0] // span
    for g in range(0, rows, group):
        part = slab_ref[g : g + group].reshape(group * span, columns)
        moved = jnp.dot(select_ref[...], part, preferred_element_type=jnp.float32)
        moved = moved.astype(jnp.bfloat16).reshape(span, group, columns)
        for (a0, a1, f0, f1), out_ref in zip(chunks, out_refs):
            out_ref[0, :, g : g + group, :] = moved[f0:f1, :, a0:a1]


def pack(w_vvv, virts, roots, root, chunks):
    rows, total, columns = w_vvv.shape
    span = total // (virts * roots)
    group = 16
    if span % 16 or rows % group or any((a1 - a0) % 128 for a0, a1, _, _ in chunks):
        slab = w_vvv.reshape(rows, virts, roots, span, columns)
        slab = lax.dynamic_index_in_dim(slab, root, 2, keepdims=False).transpose(1, 2, 0, 3)
        return [slab[:, f0:f1, :, a0:a1] for a0, a1, f0, f1 in chunks]
    to = np.arange(span * group)[:, None]
    select = np.arange(span * group)[None] == to % group * span + to // group
    shapes = [(virts, f1 - f0, rows, a1 - a0) for a0, a1, f0, f1 in chunks]
    return pl.pallas_call(
        functools.partial(pack_body, chunks=chunks),
        grid_spec=pltpu.PrefetchScalarGridSpec(
            num_scalar_prefetch=1,
            grid=(virts,),
            in_specs=[
                pl.BlockSpec(select.shape, lambda i, q: (0, 0)),
                pl.BlockSpec((rows, span, columns), lambda i, q: (0, i * roots + q[0], 0)),
            ],
            out_specs=[pl.BlockSpec((1, *shape[1:]), lambda i, q: (i, 0, 0, 0)) for shape in shapes],
        ),
        out_shape=[jax.ShapeDtypeStruct(shape, w_vvv.dtype) for shape in shapes],
        cost_estimate=pl.CostEstimate(
            flops=2 * virts * span * rows * columns * span * group,
            bytes_accessed=4 * virts * rows * span * columns,
            transcendentals=0,
        ),
    )(root[None].astype(jnp.int32), jnp.asarray(select, w_vvv.dtype), w_vvv)


def ladder_body(place_ref, tau_ref, *refs, steps, count):
    pieces, out_ref, left_ref = refs[:count], refs[-2], refs[-1]
    at = pl.program_id(0)

    @pl.when(at == 0)
    def _():
        out_ref[...] = refs[count][...] if len(refs) > count + 2 else jnp.zeros_like(out_ref)

    for k, piece_ref in enumerate(pieces):

        @pl.when(at // steps == k)
        def _(piece_ref=piece_ref):
            sources, taken, rows, columns = piece_ref.shape
            left = [piece_ref[:, f].reshape(sources * rows, columns) for f in range(taken)]
            left_ref[...] = jnp.concatenate(left, 0)

    right = tau_ref[...].reshape(left_ref.shape[0], tau_ref.shape[-1])
    out_ref[...] += lax.dot_general(
        left_ref[...], right, (((0,), (0,)), ((), ())), preferred_element_type=jnp.float32
    )


def ladder(tau, pieces, running, places, first, roots):
    sources, taken, rows, columns = pieces[0].shape
    total, pairs = tau.shape[1:]
    span = tau.shape[0] // roots
    count = len(pieces)
    step = 4
    while taken % step or first % step or span % step:
        step //= 2
    steps = taken // step
    whole = pl.BlockSpec((columns, pairs), lambda i, q: (0, 0))
    given = () if running is None else (running,)

    def piece_spec(k):
        return pl.BlockSpec(
            (sources, step, rows, columns),
            lambda i, q: (0, jnp.clip(i - k * steps, 0, steps - 1), 0, 0),
        )

    return pl.pallas_call(
        functools.partial(ladder_body, steps=steps, count=count),
        grid_spec=pltpu.PrefetchScalarGridSpec(
            num_scalar_prefetch=1,
            grid=(count * steps,),
            in_specs=[
                pl.BlockSpec(
                    (step, total, pairs),
                    lambda i, q: (q[i // steps] + i % steps, 0, 0),
                ),
                *[piece_spec(k) for k in range(count)],
                *[whole for _ in given],
            ],
            out_specs=whole,
            scratch_shapes=[pltpu.VMEM((step * sources * rows, columns), tau.dtype)],
        ),
        out_shape=jax.ShapeDtypeStruct((columns, pairs), jnp.float32),
        input_output_aliases={2 + count: 0} if given else {},
        cost_estimate=pl.CostEstimate(
            flops=2 * count * sources * taken * rows * columns * pairs,
            bytes_accessed=2 * count * sources * taken * rows * (columns + pairs),
            transcendentals=0,
        ),
    )((jnp.stack(places).astype(jnp.int32) * span + first) // step, tau, *pieces, *given)


def on_device(sizes, r2, tau, w_vvv, w_oooo, w_ovoo, fock_oo, fock_vv, r1):
    roots, virts = sizes["root"], sizes["virt"]
    root, virt = lax.axis_index("root"), lax.axis_index("virt")
    f32 = jnp.float32
    block, _, columns = w_vvv.shape
    fblock, _, pairs = tau.shape
    occupied = fock_oo.shape[0]
    pair_rows = w_oooo.shape[0]
    rq = pair_rows // roots

    def exchange(send):
        parts = []
        for key in range(virts):
            piece = lax.dynamic_index_in_dim(send, virt ^ key, 0)
            if key:
                piece = lax.ppermute(piece, "virt", [(k, k ^ key) for k in range(virts)])
            parts.append(piece)
        return assemble(parts, virt)

    chunks = chunks_of(columns, fblock // roots)
    sends = pack(w_vvv, virts, roots, root, list(chunks.values()))
    arrived = {}
    for name, send in zip(chunks, sends):
        if name[0] == "m":
            arrived[name] = lax.all_to_all(send, "virt", 0, 0, tiled=True)
        else:
            arrived[name] = exchange(send)

    own_rows = lax.dynamic_slice_in_dim(w_oooo, root * rq, rq, 0)
    small = jnp.concatenate([r2, own_rows], 0)
    inner = small.shape[1] // virts
    small = small.reshape(block + rq, virts, inner).transpose(1, 0, 2)
    small = exchange(small)
    r2_part = small[:, :block].reshape(columns, inner)
    rows_part = small[:, block:]
    rows_of = spread(rows_part, roots)
    oooo_part = jnp.zeros((virts, roots, rq, inner), r2.dtype)
    for key, part in rows_of.items():
        oooo_part = lax.dynamic_update_slice(oooo_part, part[:, None], (0, root ^ key, 0, 0))
    oooo_part = oooo_part.reshape(pairs, inner)

    window = r2[:, :pairs]
    fock_cols = lax.dynamic_slice_in_dim(fock_vv, virt * block, block, 1)
    extra = jnp.einsum("ep,ae->pa", window, fock_cols, preferred_element_type=f32)
    outer = pairs // occupied
    cube = r2.reshape(block, occupied, occupied)
    first = jnp.einsum("mi,amj->aij", fock_oo[:, :outer], cube, preferred_element_type=f32)
    second = jnp.einsum("mj,aim->aij", fock_oo, cube[:, :outer], preferred_element_type=f32)
    occ = (first + second).reshape(block, pairs).T
    placed = lax.dynamic_update_slice(jnp.zeros((pairs, columns), f32), occ, (0, virt * block))
    extra = extra - placed
    extra = extra + jnp.einsum("pk,ak->pa", oooo_part, r2_part, preferred_element_type=f32)

    singles = jnp.dot(
        r1[None, :], w_ovoo.reshape(w_ovoo.shape[0], -1), preferred_element_type=f32
    ).reshape(pair_rows, -1)

    running = {}
    results = {}
    left = {}
    for a0, _, f0, f1 in chunks.values():
        left[a0] = left.get(a0, 0) + f1 - f0
    for name, (a0, a1, f0, f1) in chunks.items():
        held = spread(arrived[name], roots)
        for keys in groups_of(name, roots):
            running[a0] = ladder(
                tau, [held[k] for k in keys], running.get(a0), [root ^ k for k in keys], f0, roots
            )
        left[a0] -= f1 - f0
        if not left[a0]:
            partial = running[a0].T + extra[:, a0:a1]
            summed = scatter_sum(partial.reshape(virts, pair_rows, a1 - a0), virts)
            results[a0] = summed - singles[:, a0:a1]
    return jnp.concatenate([results[a0] for a0 in sorted(results)], 1)


def groups_of(name, roots):
    keys = list(range(roots))
    if name[0] == "q" or int(name[1:]) + SPLIT < len(MAIN):
        return [keys]
    return [keys[: roots // 2], keys[roots // 2 :]]


def solution(mesh):
    sizes = dict(mesh.shape)
    in_specs = (
        P("virt", "root"),
        P("virt", None, "root"),
        P("virt", None, None),
        P("virt", None),
        P(None, "virt", None),
        P(),
        P(),
        P("root"),
    )
    out_specs = P(("root", "virt"), None)

    def body(*args):
        return on_device(sizes, *args)

    return jax.shard_map(
        body, mesh=mesh, in_specs=in_specs, out_specs=out_specs, check_vma=False
    )
```
